256 devices in a mesh: expert: 64 (over x, z, core), dp: 4 (over y).
Axes of the slice: x: 4, y: 4, z: 8, core: 2. Of those that a mesh axis runs over, the one named last changes fastest.
Arguments:
- sub_inputs: bfloat16 [32768, 4096], P(('expert', 'dp')), may hold values from -6 to 6
- out_grads: bfloat16 [32768, 4096], P(('expert', 'dp')), may hold values from -6 to 6
- expert_outputs: bfloat16 [32768, 4, 2, 1024], P(('expert', 'dp')), may hold values from -6 to 6
- combine_weights: float32 [32768, 4, 2], P(('expert', 'dp')), may hold values from 0.1 to 1
- expert_ids: int32 [32768, 4, 2], P(('expert', 'dp')), may hold values from 0 to 63, as said below
- slot_ids: int32 [32768, 4, 2], P(('expert', 'dp')), may hold values from -1 to 15, as said below
- expert_input_weight: bfloat16 [64, 1024, 1024], P('expert'), may hold values from -0.1875 to 0.1875
- expert_output_weight: bfloat16 [64, 1024, 1024], P('expert'), may hold values from -0.1875 to 0.1875
Outputs:
- d_inputs: bfloat16 [32768, 4096], P(('expert', 'dp'))
- d_gates: float32 [32768, 4, 2], P(('expert', 'dp'))
- dw_in: float32 [64, 1024, 1024], P('expert', 'dp')
- dw_out: float32 [64, 1024, 1024], P('expert', 'dp')
The draws below stay inside these ranges and needn't reach their ends.
Inputs may be any that keep to these rules, and one draw needn't show every extreme that they name: `expert_ids`: the 2 experts of one sub-token differ. `slot_ids`: within the rows of one device, the kept entries that name one expert carry the slots 0, 1, 2, ... each once, so at most 16 of them; in every draw some expert has 16 kept entries from every device.
All inputs are finite; a program needn't handle non-finite values.
Results may differ from the reference program's by a relative error of at most 0.0085.
Values may be sent and summed in bfloat16 or wider, within the bound.
A program may use at most 128 MiB of HBM per device.

```python
import jax
import jax.numpy as jnp
from jax import lax

SUB = 1024
FF = 1024
HEADS = 4
TOP = 2
TOK_DEV = 128
EXPERTS = 64
CAP = 16
TOKENS = 32768
N_DP = 4


def route_tables(key):
    folded = jax.random.fold_in(key, 4111)
    key_hot, key_pick, key_near, key_spread, key_second = jax.random.split(folded, 5)
    hottest = jax.random.randint(key_hot, (), 0, EXPERTS)
    picker = jax.random.randint(key_pick, (TOKENS, HEADS), 0, 4)
    nearby = (hottest + jax.random.randint(key_near, (TOKENS, HEADS), 0, 3)) % EXPERTS
    spread = jax.random.randint(key_spread, (TOKENS, HEADS), 0, EXPERTS)
    first_choice = jnp.where(picker == 0, nearby, spread)
    row_index = (jnp.arange(TOKENS) % TOK_DEV)[:, None] * HEADS + jnp.arange(HEADS)[None, :]
    first_choice = jnp.where(row_index < CAP, hottest, first_choice)
    second_choice = (first_choice + jax.random.randint(key_second, (TOKENS, HEADS), 1, EXPERTS)) % EXPERTS
    routed = jnp.stack([first_choice, second_choice], axis=-1).astype(jnp.int32)
    blocks = TOKENS // TOK_DEV
    ordered = routed.reshape(blocks, TOK_DEV * HEADS, TOP).transpose(0, 2, 1).reshape(blocks, TOP * TOK_DEV * HEADS)

    def block_slots(block_ids):
        onehot = (block_ids[:, None] == jnp.arange(EXPERTS)[None, :]).astype(jnp.int32)
        before = jnp.cumsum(onehot, axis=0) - onehot
        return jnp.sum(before * onehot, axis=1)
    positions = lax.map(block_slots, ordered)
    slot_table = jnp.where(positions < CAP, positions, -1)
    slot_table = slot_table.reshape(blocks, TOP, TOK_DEV * HEADS).transpose(0, 2, 1).reshape(TOKENS, HEADS, TOP)
    return (routed, slot_table.astype(jnp.int32))


def draw_expert_ids(key, part):
    return route_tables(key)[0]


def draw_slot_ids(key, part):
    return route_tables(key)[1]


def level_of(rng, extent, cuts, smallest, largest):
    gain, own = 1.0, jax.random.fold_in(rng, 6)
    for position, parts in cuts:
        heights = jnp.exp(jax.random.uniform(jax.random.fold_in(own, position), (parts,), jnp.float32, smallest / len(cuts), largest / len(cuts)))
        gain = gain * jnp.repeat(heights, extent[position] // parts).reshape([-1 if axis == position else 1 for axis in range(len(extent))])
    return gain


def normal_values(key, extent, deviation, most, cuts=(), kind=jnp.bfloat16):
    drawn = jax.random.normal(key, extent, jnp.float32) * deviation
    if len(cuts) > 0:
        drawn = level_of(key, extent, cuts, -0.22, 0.18) * drawn
    return jnp.clip(drawn, min=-most, max=most).astype(kind)


def setup_inputs(seed: int = 0) -> dict:
    key_of = jax.random.split(jax.random.key(seed), 9)
    sub_inputs = normal_values(key_of[0], (TOKENS, HEADS * SUB), 1.0, 6.0, ((0, 256),))
    out_grads = normal_values(key_of[1], (TOKENS, HEADS * SUB), 1.0, 6.0, ((0, 256),))
    expert_outputs = normal_values(key_of[2], (TOKENS, HEADS, TOP, SUB), 1.0, 6.0, ((0, 256),))
    combine_weights = jnp.clip(0.1 + 0.9 * jax.random.uniform(key_of[3], (TOKENS, HEADS, TOP), jnp.float32) ** level_of(key_of[3], (TOKENS, HEADS, TOP), ((0, 256),), -0.2, 0.2), 0.1, 1.0)
    expert_ids = draw_expert_ids(jax.random.fold_in(key_of[8], 71), 0)
    slot_ids = draw_slot_ids(jax.random.fold_in(key_of[8], 71), 0)
    expert_input_weight = normal_values(key_of[6], (EXPERTS, SUB, FF), SUB ** -0.5, 0.1875, ((0, 64),))
    expert_output_weight = normal_values(key_of[7], (EXPERTS, FF, SUB), FF ** -0.5, 0.1875, ((0, 64),))
    return {"sub_inputs": sub_inputs, "out_grads": out_grads, "expert_outputs": expert_outputs, "combine_weights": combine_weights, "expert_ids": expert_ids, "slot_ids": slot_ids, "expert_input_weight": expert_input_weight, "expert_output_weight": expert_output_weight}


def reference(sub_inputs, out_grads, expert_outputs, combine_weights, expert_ids, slot_ids, expert_input_weight, expert_output_weight):
    blocks = TOKENS // TOK_DEV
    sub_rows = TOK_DEV * HEADS
    name_count = sub_rows * TOP
    kept_mask = slot_ids >= 0
    inputs_split = sub_inputs.reshape(blocks, sub_rows, SUB)
    grads_split = out_grads.reshape(blocks, sub_rows, SUB)
    outputs_split = expert_outputs.reshape(blocks, sub_rows, TOP, SUB)

    def gate_block(packed):
        grads_here, outputs_here = packed
        return jnp.einsum('ns,nks->nk', grads_here.astype(jnp.float32), outputs_here.astype(jnp.float32))
    gate_dots = lax.map(gate_block, (grads_split, outputs_split)).reshape(TOKENS, HEADS, TOP)
    d_gates = jnp.where(kept_mask, gate_dots, jnp.float32(0.0))
    weights_split = combine_weights.reshape(blocks, name_count)
    ids_flat = expert_ids.reshape(blocks, name_count).astype(jnp.int32)
    slots_flat = slot_ids.reshape(blocks, name_count).astype(jnp.int32)
    slot_target = jnp.where(slots_flat >= 0, slots_flat, CAP).astype(jnp.int32)
    block_index = jnp.broadcast_to(jnp.arange(blocks, dtype=jnp.int32)[:, None], (blocks, name_count))
    name_index = jnp.broadcast_to(jnp.arange(name_count, dtype=jnp.int32)[None, :], (blocks, name_count))
    owner_table = jnp.full((blocks, EXPERTS, CAP), -1, jnp.int32)
    owner_table = owner_table.at[block_index, ids_flat, slot_target].set(name_index, mode='drop')

    def replica_sum(left, right):
        groups = blocks // N_DP
        left_split = left.reshape(groups, N_DP, CAP, left.shape[-1]).astype(jnp.float32)
        right_split = right.reshape(groups, N_DP, CAP, right.shape[-1]).astype(jnp.float32)
        partial_value = jnp.einsum('gdca,gdcb->dab', left_split, right_split).astype(jnp.bfloat16)
        partial_value = lax.optimization_barrier(partial_value)
        return lax.optimization_barrier(jnp.sum(partial_value.astype(jnp.float32), axis=0))

    def expert_grads(expert):
        picked = owner_table[:, expert, :]
        present = picked >= 0
        safe_index = jnp.maximum(picked, 0).astype(jnp.int32)
        source = (safe_index // TOP).astype(jnp.int32)
        inputs_here = jnp.take_along_axis(inputs_split, source[:, :, None], axis=1)
        grads_here = jnp.take_along_axis(grads_split, source[:, :, None], axis=1)
        weight_here = jnp.take_along_axis(weights_split, safe_index, axis=1)
        inputs_here = jnp.where(present[:, :, None], inputs_here, jnp.zeros((), jnp.bfloat16))
        inputs_here = inputs_here.astype(jnp.bfloat16).reshape(blocks * CAP, SUB)
        upstream = jnp.where(present[:, :, None], weight_here[:, :, None] * grads_here.astype(jnp.float32), jnp.float32(0.0))
        upstream = upstream.astype(jnp.bfloat16).reshape(blocks * CAP, SUB)
        weight_in = expert_input_weight[expert]
        weight_out = expert_output_weight[expert]
        preactivation_value = jnp.dot(inputs_here, weight_in, preferred_element_type=jnp.float32)
        hidden_activation, gelu_back = jax.vjp(jax.nn.gelu, preactivation_value)
        hidden_activation = hidden_activation.astype(jnp.bfloat16)
        hidden_grad = jnp.dot(upstream, weight_out.T, preferred_element_type=jnp.float32)
        preactivation_gradient = gelu_back(hidden_grad)[0].astype(jnp.bfloat16)
        grad_out = replica_sum(hidden_activation, upstream)
        grad_in = replica_sum(inputs_here, preactivation_gradient)
        input_grad = jnp.dot(preactivation_gradient, weight_in.T, preferred_element_type=jnp.float32).astype(jnp.bfloat16)
        return (grad_in, grad_out, input_grad.reshape(blocks, CAP, SUB))
    dw_in, dw_out, returned = lax.map(expert_grads, jnp.arange(EXPERTS, dtype=jnp.int32))
    returned_rows = returned.reshape(EXPERTS * blocks * CAP, SUB)

    def merge_block(packed):
        ids_here, slots_here, which_block = packed
        flat_index = (ids_here * blocks + which_block) * CAP + slots_here
        flat_index = jnp.where(slots_here >= 0, flat_index, 0).astype(jnp.int32)
        rows_here = returned_rows[flat_index].astype(jnp.float32)
        rows_here = jnp.where((slots_here >= 0)[:, None], rows_here, jnp.float32(0.0))
        return lax.optimization_barrier(jnp.sum(rows_here.reshape(sub_rows, TOP, SUB), axis=1)).astype(jnp.bfloat16)
    merged = lax.map(merge_block, (ids_flat, slots_flat, jnp.arange(blocks, dtype=jnp.int32)))
    d_inputs = merged.reshape(TOKENS, HEADS * SUB)
    return (d_inputs, d_gates, dw_in, dw_out)
```

```python
import functools
import math

import jax
import jax.numpy as jnp
from jax import lax
from jax.experimental import pallas as pl
from jax.experimental.pallas import tpu as pltpu
from jax.sharding import PartitionSpec as P

MESH = pl.DeviceIdType.MESH
NX, NZ, NC = 4, 8, 2
NY = 4
CAP = 16
PEERS = NX * NC
ROWS = PEERS * CAP
GELU_C = math.sqrt(2.0 / math.pi)
NT = (((1,), (1,)), ((), ()))
TN = (((0,), (0,)), ((), ()))
F32, BF16 = jnp.float32, jnp.bfloat16


def kernel(
    x_hbm, g_hbm, eo_hbm, w_ref, ids_ref, slots_ref, w1_hbm, w2_hbm,
    din_ref, dgate_ref, dwin_ref, dwout_ref,
    xs, gs, eo, w1, w2, tgt, onehot, send, recv, hid, grad, rsend, rrecv, acc,
    part, opp, fwd, direct,
    load_sem, send_sem, recv_sem, rsend_sem, rrecv_sem, y_send, y_opp, y_dir,
):
    sub = w1.shape[0]
    tok = xs.shape[0] // 4
    e, y = lax.axis_index("expert"), lax.axis_index("dp")
    x, z, c = e // (NZ * NC), lax.rem(e // NC, NZ), lax.rem(e, NC)
    up, down = lax.rem(y + 1, NY), lax.rem(y + NY - 1, NY)

    loads = []
    for src, dst, k in ((x_hbm, xs, 0), (g_hbm, gs, 1)):
        for h in range(4):
            loads.append(
                pltpu.make_async_copy(
                    src.at[:, h * sub:(h + 1) * sub], dst.at[pl.ds(h * tok, tok)], load_sem.at[k, h]
                )
            )
    late = [
        pltpu.make_async_copy(w1_hbm, w1, load_sem.at[2, 0]),
        pltpu.make_async_copy(w2_hbm, w2, load_sem.at[2, 1]),
        pltpu.make_async_copy(eo_hbm, eo, load_sem.at[2, 2]),
    ]
    for copy in loads + late:
        copy.start()

    barrier = pltpu.get_barrier_semaphore()

    def greet(k, _):
        pl.semaphore_signal(barrier, inc=1, device_id=(lax.rem(e + k, NX * NZ * NC), y), device_id_type=MESH)
        return 0

    lax.fori_loop(1, NX * NZ * NC, greet, 0)
    for other in (up, down):
        pl.semaphore_signal(barrier, inc=1, device_id=(e, other), device_id_type=MESH)

    tgt[...] = jnp.where(slots_ref[...] >= 0, ids_ref[...] * CAP + slots_ref[...], -1)

    def offset_z(j):
        half = (j + 1) // 2
        return lax.rem(NZ // 2 + half * (1 - 2 * lax.rem(j, 2)), NZ)

    def build(j):
        dz = offset_z(j)
        row = lax.broadcasted_iota(jnp.int32, (ROWS, tok), 0)
        px = (x + (row >> 5)) & (NX - 1)
        pz = lax.rem(z + dz, NZ)
        pc = (c + ((row >> 4) & 1)) & 1
        slot = (((px * NZ) + pz) * NC + pc) * CAP + (row & (CAP - 1))
        scale = jnp.zeros((ROWS, tok), F32)
        for h in range(4):
            first = tgt[h, 0:1, :] == slot
            second = tgt[h, 1:2, :] == slot
            onehot[j, :, h * tok:(h + 1) * tok] = jnp.where(first | second, 1.0, 0.0).astype(BF16)
            scale = scale + jnp.where(first, w_ref[h, 0:1, :], 0.0) + jnp.where(second, w_ref[h, 1:2, :], 0.0)
        scale = jnp.sum(scale, axis=1, keepdims=True)
        pick = onehot[j]
        rows_x = jnp.dot(pick, xs[...], preferred_element_type=F32).astype(BF16)
        rows_g = (jnp.dot(pick, gs[...], preferred_element_type=F32) * scale).astype(BF16)
        send[j, :, 0] = rows_x.reshape(PEERS, CAP, sub)
        send[j, :, 1] = rows_g.reshape(PEERS, CAP, sub)

    def peer(j, i, sign):
        dz, dx, dc = offset_z(j), i // NC, i % NC
        px = lax.rem(x + NX + sign * dx, NX)
        pz = lax.rem(z + NZ + sign * dz, NZ)
        return ((px * NZ) + pz) * NC + lax.rem(c + dc, NC)

    def out_copy(j, i):
        return pltpu.make_async_remote_copy(
            src_ref=send.at[j, i], dst_ref=recv.at[j, i], send_sem=send_sem.at[j], recv_sem=recv_sem.at[j],
            device_id=(peer(j, i, 1), y), device_id_type=MESH,
        )

    def back_copy(j, i):
        return pltpu.make_async_remote_copy(
            src_ref=rsend.at[j, i], dst_ref=rrecv.at[j, i], send_sem=rsend_sem.at[j], recv_sem=rrecv_sem.at[j],
            device_id=(peer(j, i, -1), y), device_id_type=MESH,
        )

    last = NZ - 1

    def ship(j, copy):
        @pl.when(j < last)
        def _():
            copy(j, 0).start()

        for i in range(1, PEERS):
            copy(j, i).start()

    def settle(j, buf, sem):
        @pl.when(j < last)
        def _():
            pltpu.make_async_copy(buf.at[j], buf.at[j], sem.at[j]).wait()

        @pl.when(j == last)
        def _():
            own = buf.at[j, pl.ds(1, PEERS - 1)]
            pltpu.make_async_copy(own, own, sem.at[j]).wait()

    for copy in loads:
        copy.wait()
    build(0)
    pl.semaphore_wait(barrier, NX * NZ * NC - 1 + 2)

    def dispatch(j, _):
        build(j)
        ship(j - 1, out_copy)
        return 0

    lax.fori_loop(1, NZ, dispatch, 0)
    recv[last, 0] = send[last, 0]
    ship(last, out_copy)

    late[2].wait()
    for h in range(4):
        mine = eo[:, h].reshape(2 * tok, sub)
        dots = lax.dot_general(mine, gs[h * tok:(h + 1) * tok, :], NT, preferred_element_type=F32)
        row = lax.broadcasted_iota(jnp.int32, (2 * tok, tok), 0)
        col = lax.broadcasted_iota(jnp.int32, (2 * tok, tok), 1)
        for k in range(2):
            kept = jnp.sum(jnp.where(row == 2 * col + k, dots, 0.0), axis=0, keepdims=True)
            dgate_ref[h, k:k + 1, :] = jnp.where(slots_ref[h, k:k + 1, :] >= 0, kept, 0.0)
    late[0].wait()
    late[1].wait()

    def experts(j, _):
        settle(j, recv, recv_sem)
        rows_x = recv[j, :, 0].reshape(ROWS, sub)
        rows_g = recv[j, :, 1].reshape(ROWS, sub)
        v = jnp.dot(rows_x, w1[...], preferred_element_type=F32)
        d = lax.dot_general(rows_g, w2[...], NT, preferred_element_type=F32)
        square = v * v
        t = jnp.tanh(GELU_C * (v + 0.044715 * (square * v)))
        cdf = 0.5 * (1.0 + t)
        slope = cdf + (0.5 * v) * (1.0 - t * t) * (GELU_C * (1.0 + (3 * 0.044715) * square))
        f = (d * slope).astype(BF16)
        r = lax.dot_general(f, w1[...], NT, preferred_element_type=F32).astype(BF16)
        rsend[j] = r.reshape(PEERS, CAP, sub)
        at = pl.ds(pl.multiple_of(j * ROWS, ROWS), ROWS)
        grad[at, :] = f
        hid[at, :] = (v * cdf).astype(BF16)
        ship(j, back_copy)
        return 0

    lax.fori_loop(0, NZ, experts, 0)
    rrecv[last, 0] = rsend[last, 0]

    quarter = sub // NY
    half = quarter // 2

    def quarter_of(a, k):
        cols = pl.ds(pl.multiple_of(lax.rem(y + k, NY) * quarter, quarter), quarter)
        if a == 0:
            left, right = hid[:, cols], recv[:, :, 1].reshape(NZ * ROWS, sub)
        else:
            left, right = recv[:, :, 0, :, cols].reshape(NZ * ROWS, quarter), grad[...]
        part[a, k] = lax.dot_general(left, right, TN, preferred_element_type=F32).astype(BF16)

    def along(src, dst, s_sem, r_sem, to):
        return pltpu.make_async_remote_copy(
            src_ref=src, dst_ref=dst, send_sem=s_sem, recv_sem=r_sem, device_id=(e, to), device_id_type=MESH
        )

    ups, downs = pl.ds(0, half), pl.ds(half, half)
    first_up = [along(part.at[a, 2, ups], opp.at[a, 0], y_send.at[0, a], y_opp.at[a, 0], up) for a in range(2)]
    first_down = [along(part.at[a, 2, downs], opp.at[a, 1], y_send.at[1, a], y_opp.at[a, 1], down) for a in range(2)]
    plain_up = [along(part.at[a, 1, downs], direct.at[a, 0, downs], y_send.at[2, a], y_dir.at[a, 0], up) for a in range(2)]
    plain_down = [along(part.at[a, 3, ups], direct.at[a, 1, ups], y_send.at[3, a], y_dir.at[a, 1], down) for a in range(2)]
    second_up = [along(fwd.at[a, 0], direct.at[a, 0, ups], y_send.at[4, a], y_dir.at[a, 2], up) for a in range(2)]
    second_down = [along(fwd.at[a, 1], direct.at[a, 1, downs], y_send.at[5, a], y_dir.at[a, 3], down) for a in range(2)]

    quarter_of(0, 2)
    quarter_of(1, 2)
    for a in range(2):
        first_up[a].start()
        first_down[a].start()
    for k in (1, 3):
        for a in range(2):
            quarter_of(a, k)
    for a in range(2):
        plain_up[a].start()
        plain_down[a].start()
    for a in range(2):
        quarter_of(a, 0)
    for a in range(2):
        first_up[a].wait_recv()
        fwd[a, 0] = (part[a, 1, ups].astype(F32) + opp[a, 0].astype(F32)).astype(BF16)
        first_down[a].wait_recv()
        fwd[a, 1] = (part[a, 3, downs].astype(F32) + opp[a, 1].astype(F32)).astype(BF16)
    for a in range(2):
        second_up[a].start()
        second_down[a].start()

    acc[...] = jnp.zeros_like(acc)

    def merge(j, _):
        settle(j, rrecv, rrecv_sem)
        rows = rrecv[j].reshape(ROWS, sub)
        acc[...] += lax.dot_general(onehot[j], rows, TN, preferred_element_type=F32)
        return 0

    lax.fori_loop(0, NZ, merge, 0)
    for h in range(4):
        din_ref[:, h * sub:(h + 1) * sub] = acc[h * tok:(h + 1) * tok, :].astype(BF16)

    for a, out in ((0, dwout_ref), (1, dwin_ref)):
        plain_up[a].wait_recv()
        plain_down[a].wait_recv()
        second_up[a].wait_recv()
        second_down[a].wait_recv()
        out[...] = part[a, 0].astype(F32) + (direct[a, 0].astype(F32) + direct[a, 1].astype(F32))

    def drain(j, _):
        settle(j, send, send_sem)
        settle(j, rsend, rsend_sem)
        return 0

    lax.fori_loop(0, NZ, drain, 0)
    for copy in first_up + first_down + plain_up + plain_down + second_up + second_down:
        copy.wait_send()


def on_device(x, g, eo, w, ids, slots, w1, w2):
    tok, width = x.shape
    sub = w1.shape[1]
    heads = width // sub
    names = tok * heads
    total = NZ * ROWS
    quarter = sub // NY
    vmem = pl.BlockSpec(memory_space=pltpu.VMEM)
    hbm = pl.BlockSpec(memory_space=pl.ANY)
    lanes = lambda v: jnp.transpose(v, (1, 2, 0))
    d_in, d_gates, dw_in, dw_out = pl.pallas_call(
        kernel,
        name="moe_backward",
        out_shape=(
            jax.ShapeDtypeStruct((tok, width), BF16),
            jax.ShapeDtypeStruct((heads, 2, tok), F32),
            jax.ShapeDtypeStruct((quarter, sub), F32),
            jax.ShapeDtypeStruct((quarter, sub), F32),
        ),
        in_specs=[hbm, hbm, hbm, vmem, vmem, vmem, hbm, hbm],
        out_specs=(vmem, vmem, vmem, vmem),
        scratch_shapes=[
            pltpu.VMEM((names, sub), BF16),
            pltpu.VMEM((names, sub), BF16),
            pltpu.VMEM((tok, heads, 2, sub), BF16),
            pltpu.VMEM((sub, sub), BF16),
            pltpu.VMEM((sub, sub), BF16),
            pltpu.VMEM((heads, 2, tok), jnp.int32),
            pltpu.VMEM((NZ, ROWS, names), BF16),
            pltpu.VMEM((NZ, PEERS, 2, CAP, sub), BF16),
            pltpu.VMEM((NZ, PEERS, 2, CAP, sub), BF16),
            pltpu.VMEM((total, sub), BF16),
            pltpu.VMEM((total, sub), BF16),
            pltpu.VMEM((NZ, PEERS, CAP, sub), BF16),
            pltpu.VMEM((NZ, PEERS, CAP, sub), BF16),
            pltpu.VMEM((names, sub), F32),
            pltpu.VMEM((2, NY, quarter, sub), BF16),
            pltpu.VMEM((2, 2, quarter // 2, sub), BF16),
            pltpu.VMEM((2, 2, quarter // 2, sub), BF16),
            pltpu.VMEM((2, 2, quarter, sub), BF16),
            pltpu.SemaphoreType.DMA((3, 4)),
            pltpu.SemaphoreType.DMA((NZ,)),
            pltpu.SemaphoreType.DMA((NZ,)),
            pltpu.SemaphoreType.DMA((NZ,)),
            pltpu.SemaphoreType.DMA((NZ,)),
            pltpu.SemaphoreType.DMA((6, 2)),
            pltpu.SemaphoreType.DMA((2, 2)),
            pltpu.SemaphoreType.DMA((2, 4)),
        ],
        compiler_params=pltpu.CompilerParams(collective_id=0, has_side_effects=True, vmem_limit_bytes=62 << 20),
    )(x, g, eo, lanes(w), lanes(ids), lanes(slots), w1.reshape(sub, sub), w2.reshape(sub, sub))
    return d_in, jnp.transpose(d_gates, (2, 0, 1)), dw_in[None], dw_out[None]


def solution(mesh):
    tokens = P(("expert", "dp"), None)
    per_entry = P(("expert", "dp"), None, None)
    weights = P("expert", None, None)
    in_specs = (tokens, tokens, P(("expert", "dp"), None, None, None)) + (per_entry,) * 3 + (weights,) * 2
    out_specs = (tokens, per_entry, P("expert", "dp", None), P("expert", "dp", None))
    return jax.shard_map(on_device, mesh=mesh, in_specs=in_specs, out_specs=out_specs, check_vma=False)
```

```python
import functools
import math

import jax
import jax.numpy as jnp
from jax import lax
from jax.experimental import pallas as pl
from jax.experimental.pallas import tpu as pltpu
from jax.sharding import PartitionSpec as P

MESH = pl.DeviceIdType.MESH
NX, NZ, NC = 4, 8, 2
NY = 4
CAP = 16
PEERS = NX * NC
ROWS = PEERS * CAP
GELU_C = math.sqrt(2.0 / math.pi)
NT = (((1,), (1,)), ((), ()))
TN = (((0,), (0,)), ((), ()))
F32, BF16 = jnp.float32, jnp.bfloat16


def kernel(
    x_hbm, g_hbm, eo_hbm, w_ref, ids_ref, slots_ref, w1_hbm, w2_hbm,
    din_ref, dgate_ref, dwin_ref, dwout_ref,
    xs, gs, eo, w1, w2, tgt, onehot, send, recv, hid, grad, rsend, rrecv, acc,
    part, opp, fwd, direct,
    load_sem, send_sem, recv_sem, rsend_sem, rrecv_sem, y_send, y_opp, y_dir,
):
    sub = w1.shape[0]
    tok = xs.shape[0] // 4
    e, y = lax.axis_index("expert"), lax.axis_index("dp")
    x, z, c = e // (NZ * NC), lax.rem(e // NC, NZ), lax.rem(e, NC)
    up, down = lax.rem(y + 1, NY), lax.rem(y + NY - 1, NY)

    loads = []
    for src, dst, k in ((x_hbm, xs, 0), (g_hbm, gs, 1)):
        for h in range(4):
            loads.append(
                pltpu.make_async_copy(
                    src.at[:, h * sub:(h + 1) * sub], dst.at[pl.ds(h * tok, tok)], load_sem.at[k, h]
                )
            )
    late = [
        pltpu.make_async_copy(w1_hbm, w1, load_sem.at[2, 0]),
        pltpu.make_async_copy(w2_hbm, w2, load_sem.at[2, 1]),
        pltpu.make_async_copy(eo_hbm, eo, load_sem.at[2, 2]),
    ]
    for copy in loads:
        copy.start()

    barrier = pltpu.get_barrier_semaphore()

    def greet(k, _):
        pl.semaphore_signal(barrier, inc=1, device_id=(lax.rem(e + k, NX * NZ * NC), y), device_id_type=MESH)
        return 0

    lax.fori_loop(1, NX * NZ * NC, greet, 0)
    for other in (up, down):
        pl.semaphore_signal(barrier, inc=1, device_id=(e, other), device_id_type=MESH)

    tgt[...] = jnp.where(slots_ref[...] >= 0, ids_ref[...] * CAP + slots_ref[...], -1)

    def offset_z(j):
        k = NZ - 1 - j
        half = (k + 1) // 2
        return lax.rem(NZ // 2 + half * (1 - 2 * lax.rem(k, 2)), NZ)

    def build(j):
        dz = offset_z(j)
        row = lax.broadcasted_iota(jnp.int32, (ROWS, tok), 0)
        px = (x + (row >> 5)) & (NX - 1)
        pz = lax.rem(z + dz, NZ)
        pc = (c + ((row >> 4) & 1)) & 1
        slot = (((px * NZ) + pz) * NC + pc) * CAP + (row & (CAP - 1))
        scale = jnp.zeros((ROWS, tok), F32)
        for h in range(4):
            first = tgt[h, 0:1, :] == slot
            second = tgt[h, 1:2, :] == slot
            onehot[j, :, h * tok:(h + 1) * tok] = jnp.where(first | second, 1.0, 0.0).astype(BF16)
            scale = scale + jnp.where(first, w_ref[h, 0:1, :], 0.0) + jnp.where(second, w_ref[h, 1:2, :], 0.0)
        scale = jnp.sum(scale, axis=1, keepdims=True)
        pick = onehot[j]
        rows_x = jnp.dot(pick, xs[...], preferred_element_type=F32).astype(BF16)
        rows_g = (jnp.dot(pick, gs[...], preferred_element_type=F32) * scale).astype(BF16)
        send[j, :, 0] = rows_x.reshape(PEERS, CAP, sub)
        send[j, :, 1] = rows_g.reshape(PEERS, CAP, sub)

    def peer(j, i, sign):
        dz, dx, dc = offset_z(j), i // NC, i % NC
        px = lax.rem(x + NX + sign * dx, NX)
        pz = lax.rem(z + NZ + sign * dz, NZ)
        return ((px * NZ) + pz) * NC + lax.rem(c + dc, NC)

    def out_copy(j, i):
        return pltpu.make_async_remote_copy(
            src_ref=send.at[j, i], dst_ref=recv.at[j, i], send_sem=send_sem.at[j], recv_sem=recv_sem.at[j],
            device_id=(peer(j, i, 1), y), device_id_type=MESH,
        )

    def back_copy(j, i):
        return pltpu.make_async_remote_copy(
            src_ref=rsend.at[j, i], dst_ref=rrecv.at[j, i], send_sem=rsend_sem.at[j], recv_sem=rrecv_sem.at[j],
            device_id=(peer(j, i, -1), y), device_id_type=MESH,
        )

    home = 0

    def ship(j, copy):
        @pl.when(j != home)
        def _():
            copy(j, 0).start()

        for i in range(1, PEERS):
            copy(j, i).start()

    def settle(j, buf, sem):
        @pl.when(j != home)
        def _():
            pltpu.make_async_copy(buf.at[j], buf.at[j], sem.at[j]).wait()

        @pl.when(j == home)
        def _():
            own = buf.at[j, pl.ds(1, PEERS - 1)]
            pltpu.make_async_copy(own, own, sem.at[j]).wait()

    for copy in loads:
        copy.wait()
    build(0)
    for copy in late:
        copy.start()
    pl.semaphore_wait(barrier, NX * NZ * NC - 1 + 2)
    ship(0, out_copy)
    build(1)

    def dispatch(j, _):
        build(j)
        ship(j - 1, out_copy)
        return 0

    lax.fori_loop(2, NZ, dispatch, 0)
    recv[home, 0] = send[home, 0]
    ship(NZ - 1, out_copy)

    late[2].wait()
    for h in range(4):
        mine = eo[:, h].reshape(2 * tok, sub)
        dots = lax.dot_general(mine, gs[h * tok:(h + 1) * tok, :], NT, preferred_element_type=F32)
        row = lax.broadcasted_iota(jnp.int32, (2 * tok, tok), 0)
        col = lax.broadcasted_iota(jnp.int32, (2 * tok, tok), 1)
        for k in range(2):
            kept = jnp.sum(jnp.where(row == 2 * col + k, dots, 0.0), axis=0, keepdims=True)
            dgate_ref[h, k:k + 1, :] = jnp.where(slots_ref[h, k:k + 1, :] >= 0, kept, 0.0)
    late[0].wait()
    late[1].wait()

    def experts(j, _):
        settle(j, recv, recv_sem)
        rows_x = recv[j, :, 0].reshape(ROWS, sub)
        rows_g = recv[j, :, 1].reshape(ROWS, sub)
        v = jnp.dot(rows_x, w1[...], preferred_element_type=F32)
        d = lax.dot_general(rows_g, w2[...], NT, preferred_element_type=F32)
        square = v * v
        t = jnp.tanh(GELU_C * (v + 0.044715 * (square * v)))
        cdf = 0.5 * (1.0 + t)
        slope = cdf + (0.5 * v) * (1.0 - t * t) * (GELU_C * (1.0 + (3 * 0.044715) * square))
        f = (d * slope).astype(BF16)
        r = lax.dot_general(f, w1[...], NT, preferred_element_type=F32).astype(BF16)
        rsend[j] = r.reshape(PEERS, CAP, sub)
        at = pl.ds(pl.multiple_of(j * ROWS, ROWS), ROWS)
        grad[at, :] = f
        hid[at, :] = (v * cdf).astype(BF16)
        ship(j, back_copy)
        return 0

    lax.fori_loop(0, NZ, experts, 0)
    rrecv[home, 0] = rsend[home, 0]

    quarter = sub // NY
    half = quarter // 2

    def quarter_of(a, k):
        cols = pl.ds(pl.multiple_of(lax.rem(y + k, NY) * quarter, quarter), quarter)
        if a == 0:
            left, right = hid[:, cols], recv[:, :, 1].reshape(NZ * ROWS, sub)
        else:
            left, right = recv[:, :, 0, :, cols].reshape(NZ * ROWS, quarter), grad[...]
        part[a, k] = lax.dot_general(left, right, TN, preferred_element_type=F32).astype(BF16)

    def along(src, dst, s_sem, r_sem, to):
        return pltpu.make_async_remote_copy(
            src_ref=src, dst_ref=dst, send_sem=s_sem, recv_sem=r_sem, device_id=(e, to), device_id_type=MESH
        )

    ups, downs = pl.ds(0, half), pl.ds(half, half)
    first_up = [along(part.at[a, 2, ups], opp.at[a, 0], y_send.at[0, a], y_opp.at[a, 0], up) for a in range(2)]
    first_down = [along(part.at[a, 2, downs], opp.at[a, 1], y_send.at[1, a], y_opp.at[a, 1], down) for a in range(2)]
    plain_up = [along(part.at[a, 1, downs], direct.at[a, 0, downs], y_send.at[2, a], y_dir.at[a, 0], up) for a in range(2)]
    plain_down = [along(part.at[a, 3, ups], direct.at[a, 1, ups], y_send.at[3, a], y_dir.at[a, 1], down) for a in range(2)]
    second_up = [along(fwd.at[a, 0], direct.at[a, 0, ups], y_send.at[4, a], y_dir.at[a, 2], up) for a in range(2)]
    second_down = [along(fwd.at[a, 1], direct.at[a, 1, downs], y_send.at[5, a], y_dir.at[a, 3], down) for a in range(2)]

    quarter_of(0, 2)
    quarter_of(1, 2)
    for a in range(2):
        first_up[a].start()
        first_down[a].start()
    for k in (1, 3):
        for a in range(2):
            quarter_of(a, k)
    for a in range(2):
        plain_up[a].start()
        plain_down[a].start()
    for a in range(2):
        quarter_of(a, 0)
    for a in range(2):
        first_up[a].wait_recv()
        fwd[a, 0] = (part[a, 1, ups].astype(F32) + opp[a, 0].astype(F32)).astype(BF16)
        first_down[a].wait_recv()
        fwd[a, 1] = (part[a, 3, downs].astype(F32) + opp[a, 1].astype(F32)).astype(BF16)
    for a in range(2):
        second_up[a].start()
        second_down[a].start()

    acc[...] = jnp.zeros_like(acc)

    def merge(j, _):
        settle(j, rrecv, rrecv_sem)
        rows = rrecv[j].reshape(ROWS, sub)
        acc[...] += lax.dot_general(onehot[j], rows, TN, preferred_element_type=F32)
        return 0

    lax.fori_loop(0, NZ, merge, 0)
    for h in range(4):
        din_ref[:, h * sub:(h + 1) * sub] = acc[h * tok:(h + 1) * tok, :].astype(BF16)

    for a, out in ((0, dwout_ref), (1, dwin_ref)):
        plain_up[a].wait_recv()
        plain_down[a].wait_recv()
        second_up[a].wait_recv()
        second_down[a].wait_recv()
        out[...] = part[a, 0].astype(F32) + (direct[a, 0].astype(F32) + direct[a, 1].astype(F32))

    def drain(j, _):
        settle(j, send, send_sem)
        settle(j, rsend, rsend_sem)
        return 0

    lax.fori_loop(0, NZ, drain, 0)
    for copy in first_up + first_down + plain_up + plain_down + second_up + second_down:
        copy.wait_send()


def on_device(x, g, eo, w, ids, slots, w1, w2):
    tok, width = x.shape
    sub = w1.shape[1]
    heads = width // sub
    names = tok * heads
    total = NZ * ROWS
    quarter = sub // NY
    vmem = pl.BlockSpec(memory_space=pltpu.VMEM)
    hbm = pl.BlockSpec(memory_space=pltpu.HBM)
    lanes = lambda v: jnp.transpose(v, (1, 2, 0))
    d_in, d_gates, dw_in, dw_out = pl.pallas_call(
        kernel,
        name="moe_backward",
        out_shape=(
            jax.ShapeDtypeStruct((tok, width), BF16),
            jax.ShapeDtypeStruct((heads, 2, tok), F32),
            jax.ShapeDtypeStruct((quarter, sub), F32),
            jax.ShapeDtypeStruct((quarter, sub), F32),
        ),
        in_specs=[hbm, hbm, hbm, vmem, vmem, vmem, hbm, hbm],
        out_specs=(vmem, vmem, vmem, vmem),
        scratch_shapes=[
            pltpu.VMEM((names, sub), BF16),
            pltpu.VMEM((names, sub), BF16),
            pltpu.VMEM((tok, heads, 2, sub), BF16),
            pltpu.VMEM((sub, sub), BF16),
            pltpu.VMEM((sub, sub), BF16),
            pltpu.VMEM((heads, 2, tok), jnp.int32),
            pltpu.VMEM((NZ, ROWS, names), BF16),
            pltpu.VMEM((NZ, PEERS, 2, CAP, sub), BF16),
            pltpu.VMEM((NZ, PEERS, 2, CAP, sub), BF16),
            pltpu.VMEM((total, sub), BF16),
            pltpu.VMEM((total, sub), BF16),
            pltpu.VMEM((NZ, PEERS, CAP, sub), BF16),
            pltpu.VMEM((NZ, PEERS, CAP, sub), BF16),
            pltpu.VMEM((names, sub), F32),
            pltpu.VMEM((2, NY, quarter, sub), BF16),
            pltpu.VMEM((2, 2, quarter // 2, sub), BF16),
            pltpu.VMEM((2, 2, quarter // 2, sub), BF16),
            pltpu.VMEM((2, 2, quarter, sub), BF16),
            pltpu.SemaphoreType.DMA((3, 4)),
            pltpu.SemaphoreType.DMA((NZ,)),
            pltpu.SemaphoreType.DMA((NZ,)),
            pltpu.SemaphoreType.DMA((NZ,)),
            pltpu.SemaphoreType.DMA((NZ,)),
            pltpu.SemaphoreType.DMA((6, 2)),
            pltpu.SemaphoreType.DMA((2, 2)),
            pltpu.SemaphoreType.DMA((2, 4)),
        ],
        compiler_params=pltpu.CompilerParams(collective_id=0, has_side_effects=True, vmem_limit_bytes=44 << 20),
    )(x, g, eo, lanes(w), lanes(ids), lanes(slots), w1.reshape(sub, sub), w2.reshape(sub, sub))
    return d_in, jnp.transpose(d_gates, (2, 0, 1)), dw_in[None], dw_out[None]


def solution(mesh):
    tokens = P(("expert", "dp"), None)
    per_entry = P(("expert", "dp"), None, None)
    weights = P("expert", None, None)
    in_specs = (tokens, tokens, P(("expert", "dp"), None, None, None)) + (per_entry,) * 3 + (weights,) * 2
    out_specs = (tokens, per_entry, P("expert", "dp", None), P("expert", "dp", None))
    return jax.shard_map(on_device, mesh=mesh, in_specs=in_specs, out_specs=out_specs, check_vma=False)
```

```python
import functools
import math

import jax
import jax.numpy as jnp
from jax import lax
from jax.experimental import pallas as pl
from jax.experimental.pallas import tpu as pltpu
from jax.sharding import PartitionSpec as P

MESH = pl.DeviceIdType.MESH
NX, NZ, NC = 4, 8, 2
NY = 4
CAP = 16
PEERS = NX * NC
ROWS = PEERS * CAP
GELU_C = math.sqrt(2.0 / math.pi)
NT = (((1,), (1,)), ((), ()))
TN = (((0,), (0,)), ((), ()))
F32, BF16 = jnp.float32, jnp.bfloat16


def kernel(
    x_hbm, g_hbm, eo_hbm, w_hbm, ids_hbm, slots_hbm, w1_hbm, w2_hbm,
    din_ref, dgate_ref, dwin_ref, dwout_ref,
    xs, gs, eo, w1, w2, w_ref, ids_ref, slots_ref, tgt, onehot, send, recv, hid, grad, rsend, rrecv, acc,
    part, opp, fwd, direct,
    load_sem, send_sem, recv_sem, rsend_sem, rrecv_sem, y_send, y_opp, y_dir,
):
    sub = w1.shape[0]
    tok = xs.shape[0] // 4
    e, y = lax.axis_index("expert"), lax.axis_index("dp")
    x, z, c = e // (NZ * NC), lax.rem(e // NC, NZ), lax.rem(e, NC)
    up, down = lax.rem(y + 1, NY), lax.rem(y + NY - 1, NY)

    tables = [
        pltpu.make_async_copy(src, dst, load_sem.at[3, k])
        for k, (src, dst) in enumerate(((ids_hbm, ids_ref), (slots_hbm, slots_ref), (w_hbm, w_ref)))
    ]
    loads = []
    for src, dst, k in ((x_hbm, xs, 0), (g_hbm, gs, 1)):
        for h in range(4):
            loads.append(
                pltpu.make_async_copy(
                    src.at[:, h * sub:(h + 1) * sub], dst.at[pl.ds(h * tok, tok)], load_sem.at[k, h]
                )
            )
    late = [
        pltpu.make_async_copy(w1_hbm, w1, load_sem.at[2, 0]),
        pltpu.make_async_copy(w2_hbm, w2, load_sem.at[2, 1]),
        pltpu.make_async_copy(eo_hbm, eo, load_sem.at[2, 2]),
    ]
    for copy in tables + loads:
        copy.start()

    barrier = pltpu.get_barrier_semaphore()

    def greet(k, _):
        pl.semaphore_signal(barrier, inc=1, device_id=(lax.rem(e + k, NX * NZ * NC), y), device_id_type=MESH)
        return 0

    lax.fori_loop(1, NX * NZ * NC, greet, 0)
    for other in (up, down):
        pl.semaphore_signal(barrier, inc=1, device_id=(e, other), device_id_type=MESH)

    for copy in tables:
        copy.wait()
    tgt[...] = jnp.where(slots_ref[...] >= 0, ids_ref[...] * CAP + slots_ref[...], -1)

    def offset_z(j):
        k = NZ - 1 - j
        half = (k + 1) // 2
        return lax.rem(NZ // 2 + half * (1 - 2 * lax.rem(k, 2)), NZ)

    def build(j):
        dz = offset_z(j)
        row = lax.broadcasted_iota(jnp.int32, (ROWS, tok), 0)
        px = (x + (row >> 5)) & (NX - 1)
        pz = lax.rem(z + dz, NZ)
        pc = (c + ((row >> 4) & 1)) & 1
        slot = (((px * NZ) + pz) * NC + pc) * CAP + (row & (CAP - 1))
        scale = jnp.zeros((ROWS, tok), F32)
        for h in range(4):
            first = tgt[h, 0:1, :] == slot
            second = tgt[h, 1:2, :] == slot
            onehot[j, :, h * tok:(h + 1) * tok] = jnp.where(first | second, 1.0, 0.0).astype(BF16)
            scale = scale + jnp.where(first, w_ref[h, 0:1, :], 0.0) + jnp.where(second, w_ref[h, 1:2, :], 0.0)
        scale = jnp.sum(scale, axis=1, keepdims=True)
        pick = onehot[j]
        rows_x = jnp.dot(pick, xs[...], preferred_element_type=F32).astype(BF16)
        rows_g = (jnp.dot(pick, gs[...], preferred_element_type=F32) * scale).astype(BF16)
        send[j, :, 0] = rows_x.reshape(PEERS, CAP, sub)
        send[j, :, 1] = rows_g.reshape(PEERS, CAP, sub)

    def peer(j, i, sign):
        dz, dx, dc = offset_z(j), i // NC, i % NC
        px = lax.rem(x + NX + sign * dx, NX)
        pz = lax.rem(z + NZ + sign * dz, NZ)
        return ((px * NZ) + pz) * NC + lax.rem(c + dc, NC)

    def out_copy(j, i):
        return pltpu.make_async_remote_copy(
            src_ref=send.at[j, i], dst_ref=recv.at[j, i], send_sem=send_sem.at[j], recv_sem=recv_sem.at[j],
            device_id=(peer(j, i, 1), y), device_id_type=MESH,
        )

    def back_copy(j, i):
        return pltpu.make_async_remote_copy(
            src_ref=rsend.at[j, i], dst_ref=rrecv.at[j, i], send_sem=rsend_sem.at[j], recv_sem=rrecv_sem.at[j],
            device_id=(peer(j, i, -1), y), device_id_type=MESH,
        )

    home = 0

    def ship(j, copy):
        @pl.when(j != home)
        def _():
            copy(j, 0).start()

        for i in range(1, PEERS):
            copy(j, i).start()

    def settle(j, buf, sem):
        @pl.when(j != home)
        def _():
            pltpu.make_async_copy(buf.at[j], buf.at[j], sem.at[j]).wait()

        @pl.when(j == home)
        def _():
            own = buf.at[j, pl.ds(1, PEERS - 1)]
            pltpu.make_async_copy(own, own, sem.at[j]).wait()

    for copy in loads:
        copy.wait()
    build(0)
    for copy in late:
        copy.start()
    pl.semaphore_wait(barrier, NX * NZ * NC - 1 + 2)
    ship(0, out_copy)
    build(1)

    def dispatch(j, _):
        build(j)
        ship(j - 1, out_copy)
        return 0

    lax.fori_loop(2, NZ, dispatch, 0)
    recv[home, 0] = send[home, 0]
    ship(NZ - 1, out_copy)

    late[2].wait()
    for h in range(4):
        mine = eo[:, h].reshape(2 * tok, sub)
        dots = lax.dot_general(mine, gs[h * tok:(h + 1) * tok, :], NT, preferred_element_type=F32)
        row = lax.broadcasted_iota(jnp.int32, (2 * tok, tok), 0)
        col = lax.broadcasted_iota(jnp.int32, (2 * tok, tok), 1)
        for k in range(2):
            kept = jnp.sum(jnp.where(row == 2 * col + k, dots, 0.0), axis=0, keepdims=True)
            dgate_ref[h, k:k + 1, :] = jnp.where(slots_ref[h, k:k + 1, :] >= 0, kept, 0.0)
    late[0].wait()
    late[1].wait()

    def experts(j, _):
        settle(j, recv, recv_sem)
        rows_x = recv[j, :, 0].reshape(ROWS, sub)
        rows_g = recv[j, :, 1].reshape(ROWS, sub)
        v = jnp.dot(rows_x, w1[...], preferred_element_type=F32)
        d = lax.dot_general(rows_g, w2[...], NT, preferred_element_type=F32)
        square = v * v
        t = jnp.tanh(GELU_C * (v + 0.044715 * (square * v)))
        cdf = 0.5 * (1.0 + t)
        slope = cdf + (0.5 * v) * (1.0 - t * t) * (GELU_C * (1.0 + (3 * 0.044715) * square))
        f = (d * slope).astype(BF16)
        r = lax.dot_general(f, w1[...], NT, preferred_element_type=F32).astype(BF16)
        rsend[j] = r.reshape(PEERS, CAP, sub)
        at = pl.ds(pl.multiple_of(j * ROWS, ROWS), ROWS)
        grad[at, :] = f
        hid[at, :] = (v * cdf).astype(BF16)
        ship(j, back_copy)
        return 0

    lax.fori_loop(0, NZ, experts, 0)
    rrecv[home, 0] = rsend[home, 0]

    quarter = sub // NY
    half = quarter // 2

    def quarter_of(a, k):
        cols = pl.ds(pl.multiple_of(lax.rem(y + k, NY) * quarter, quarter), quarter)
        if a == 0:
            left, right = hid[:, cols], recv[:, :, 1].reshape(NZ * ROWS, sub)
        else:
            left, right = recv[:, :, 0, :, cols].reshape(NZ * ROWS, quarter), grad[...]
        part[a, k] = lax.dot_general(left, right, TN, preferred_element_type=F32).astype(BF16)

    def along(src, dst, s_sem, r_sem, to):
        return pltpu.make_async_remote_copy(
            src_ref=src, dst_ref=dst, send_sem=s_sem, recv_sem=r_sem, device_id=(e, to), device_id_type=MESH
        )

    ups, downs = pl.ds(0, half), pl.ds(half, half)
    first_up = [along(part.at[a, 2, ups], opp.at[a, 0], y_send.at[0, a], y_opp.at[a, 0], up) for a in range(2)]
    first_down = [along(part.at[a, 2, downs], opp.at[a, 1], y_send.at[1, a], y_opp.at[a, 1], down) for a in range(2)]
    plain_up = [along(part.at[a, 1, downs], direct.at[a, 0, downs], y_send.at[2, a], y_dir.at[a, 0], up) for a in range(2)]
    plain_down = [along(part.at[a, 3, ups], direct.at[a, 1, ups], y_send.at[3, a], y_dir.at[a, 1], down) for a in range(2)]
    second_up = [along(fwd.at[a, 0], direct.at[a, 0, ups], y_send.at[4, a], y_dir.at[a, 2], up) for a in range(2)]
    second_down = [along(fwd.at[a, 1], direct.at[a, 1, downs], y_send.at[5, a], y_dir.at[a, 3], down) for a in range(2)]

    quarter_of(0, 2)
    quarter_of(1, 2)
    for a in range(2):
        first_up[a].start()
        first_down[a].start()
    for k in (1, 3):
        for a in range(2):
            quarter_of(a, k)
    for a in range(2):
        plain_up[a].start()
        plain_down[a].start()
    for a in range(2):
        quarter_of(a, 0)
    for a in range(2):
        first_up[a].wait_recv()
        fwd[a, 0] = (part[a, 1, ups].astype(F32) + opp[a, 0].astype(F32)).astype(BF16)
        first_down[a].wait_recv()
        fwd[a, 1] = (part[a, 3, downs].astype(F32) + opp[a, 1].astype(F32)).astype(BF16)
    for a in range(2):
        second_up[a].start()
        second_down[a].start()

    acc[...] = jnp.zeros_like(acc)

    def merge(j, _):
        settle(j, rrecv, rrecv_sem)
        rows = rrecv[j].reshape(ROWS, sub)
        acc[...] += lax.dot_general(onehot[j], rows, TN, preferred_element_type=F32)
        return 0

    lax.fori_loop(0, NZ, merge, 0)
    for h in range(4):
        din_ref[:, h * sub:(h + 1) * sub] = acc[h * tok:(h + 1) * tok, :].astype(BF16)

    for a, out in ((0, dwout_ref), (1, dwin_ref)):
        plain_up[a].wait_recv()
        plain_down[a].wait_recv()
        second_up[a].wait_recv()
        second_down[a].wait_recv()
        out[...] = part[a, 0].astype(F32) + (direct[a, 0].astype(F32) + direct[a, 1].astype(F32))

    def drain(j, _):
        settle(j, send, send_sem)
        settle(j, rsend, rsend_sem)
        return 0

    lax.fori_loop(0, NZ, drain, 0)
    for copy in first_up + first_down + plain_up + plain_down + second_up + second_down:
        copy.wait_send()


def on_device(x, g, eo, w, ids, slots, w1, w2):
    tok, width = x.shape
    sub = w1.shape[1]
    heads = width // sub
    names = tok * heads
    total = NZ * ROWS
    quarter = sub // NY
    vmem = pl.BlockSpec(memory_space=pltpu.VMEM)
    hbm = pl.BlockSpec(memory_space=pltpu.HBM)
    lanes = lambda v: jnp.transpose(v, (1, 2, 0))
    d_in, d_gates, dw_in, dw_out = pl.pallas_call(
        kernel,
        name="moe_backward",
        out_shape=(
            pltpu.VMEM((tok, width), BF16),
            pltpu.VMEM((heads, 2, tok), F32),
            pltpu.VMEM((quarter, sub), F32),
            pltpu.VMEM((quarter, sub), F32),
        ),
        in_specs=[hbm] * 8,
        out_specs=(vmem, vmem, vmem, vmem),
        scratch_shapes=[
            pltpu.VMEM((names, sub), BF16),
            pltpu.VMEM((names, sub), BF16),
            pltpu.VMEM((tok, heads, 2, sub), BF16),
            pltpu.VMEM((sub, sub), BF16),
            pltpu.VMEM((sub, sub), BF16),
            pltpu.VMEM((heads, 2, tok), F32),
            pltpu.VMEM((heads, 2, tok), jnp.int32),
            pltpu.VMEM((heads, 2, tok), jnp.int32),
            pltpu.VMEM((heads, 2, tok), jnp.int32),
            pltpu.VMEM((NZ, ROWS, names), BF16),
            pltpu.VMEM((NZ, PEERS, 2, CAP, sub), BF16),
            pltpu.VMEM((NZ, PEERS, 2, CAP, sub), BF16),
            pltpu.VMEM((total, sub), BF16),
            pltpu.VMEM((total, sub), BF16),
            pltpu.VMEM((NZ, PEERS, CAP, sub), BF16),
            pltpu.VMEM((NZ, PEERS, CAP, sub), BF16),
            pltpu.VMEM((names, sub), F32),
            pltpu.VMEM((2, NY, quarter, sub), BF16),
            pltpu.VMEM((2, 2, quarter // 2, sub), BF16),
            pltpu.VMEM((2, 2, quarter // 2, sub), BF16),
            pltpu.VMEM((2, 2, quarter, sub), BF16),
            pltpu.SemaphoreType.DMA((4, 4)),
            pltpu.SemaphoreType.DMA((NZ,)),
            pltpu.SemaphoreType.DMA((NZ,)),
            pltpu.SemaphoreType.DMA((NZ,)),
            pltpu.SemaphoreType.DMA((NZ,)),
            pltpu.SemaphoreType.DMA((6, 2)),
            pltpu.SemaphoreType.DMA((2, 2)),
            pltpu.SemaphoreType.DMA((2, 4)),
        ],
        compiler_params=pltpu.CompilerParams(collective_id=0, has_side_effects=True, vmem_limit_bytes=54 << 20),
    )(x, g, eo, lanes(w), lanes(ids), lanes(slots), w1.reshape(sub, sub), w2.reshape(sub, sub))
    return d_in, jnp.transpose(d_gates, (2, 0, 1)), dw_in[None], dw_out[None]


def solution(mesh):
    tokens = P(("expert", "dp"), None)
    per_entry = P(("expert", "dp"), None, None)
    weights = P("expert", None, None)
    in_specs = (tokens, tokens, P(("expert", "dp"), None, None, None)) + (per_entry,) * 3 + (weights,) * 2
    out_specs = (tokens, per_entry, P("expert", "dp", None), P("expert", "dp", None))
    return jax.shard_map(on_device, mesh=mesh, in_specs=in_specs, out_specs=out_specs, check_vma=False)
```
